32 devices in a mesh: acq: 8 (over z, y), grp: 4 (over x, core).
Axes of the slice: x: 2, y: 2, z: 4, core: 2. Of those that a mesh axis runs over, the one named last changes fastest.
Arguments:
- tile_slabs: float32 [256, 16, 4096], P(('acq', 'grp')), may hold values from -6 to 6
- dest_rank: int32 [256, 1], replicated, may hold values from 0 to 7; in each aligned block of 8 rows (0 to 7, 8 to 15, ...) at most 2 rows name the same one
- block_slot: int32 [256], replicated, may hold values from 0 to 15
- shifts: float32 [256, 3], replicated, may hold values from 0 to 1
- blend_weight: float32 [256], replicated, may hold values from 0.25 to 4
- parent_map: int32 [512], P(('acq', 'grp')), may hold values from 0 to 63
Outputs:
- pyramid: float32 [64, 8, 8, 1024], P(('acq', 'grp'))
The draws below stay inside these ranges and needn't reach their ends.
Inputs may be any that keep to these rules, and one draw needn't show every extreme that they name: `dest_rank`: among the rows of one device, no acq index is named more than 2 times, a bound that some block reaches.
All inputs are finite; a program needn't handle non-finite values.
Results may differ from the reference program's by a relative error of at most 0.0003.
Values sent between devices are 32-bit elements; how exact they have to be, the bound alone decides.
A program may use at most 256 MiB of HBM per device.

```python
import math
import jax
import jax.numpy as jnp
import numpy as np
from jax import lax

BZ = 16
BY = 32
BX = 128
SB_DEV = 8
BLOCKS_DEV = 16
PAR_DEV = 2
CAP = 2
SUBS = 256
BLOCKS = 512
PARENTS = 64
N_ACQ = 8
N_GRP = 4


def with_ends(values, key, least, largest):
    dims = values.shape
    spot = [jax.random.randint(jax.random.fold_in(key, axis), (), 0, dims[axis]) for axis in range(len(dims))]
    values = values.at[tuple(spot)].set(least)
    longest = dims.index(max(dims))
    spot[longest] = (spot[longest] + 1) % dims[longest]
    return values.at[tuple(spot)].set(largest)


def block_scale(own_key, dims, pieces, least, top_value):
    loudness = 1.0
    for axis_at, shards_of in pieces:
        heights = jax.random.uniform(jax.random.fold_in(jax.random.fold_in(own_key, 6), axis_at), (shards_of,), jnp.float32, least / len(pieces), top_value / len(pieces))
        loudness = loudness * jnp.repeat(jnp.exp(heights), dims[axis_at] // shards_of).reshape((-1,) + (1,) * (len(dims) - 1 - axis_at))
    return loudness


def assign_block(stream_key, own, number, rows, number_of, top, most, slope):
    sequence = jax.random.permutation(stream_key, number_of)
    crowded, usual = load_shares(number_of, rows * top, most, slope, True), load_shares(number_of, rows * top, most, slope, False)
    places = jnp.arange(number_of)

    def named(sizes, offset_by):
        used = int((sizes > 0).sum())
        fixed = max(1, used // 4)
        moved = fixed + (places - fixed + offset_by * (used - fixed)) % max(1, number_of - fixed)
        return jnp.zeros((number_of,), jnp.int32).at[sequence[jnp.where(places < fixed, places, moved)]].set(jnp.asarray(sizes, jnp.int32))

    sizes = jnp.where(number % 4 == 0, named(crowded, number // 4), named(usual, number - number // 4 - 1))
    mixed = jax.random.permutation(jax.random.fold_in(own, 3), number_of)
    donor, receiver = mixed[0:number_of // 2 * 2:2], mixed[1:number_of // 2 * 2:2]
    margin = jnp.minimum(sizes[donor] - 1, most - sizes[receiver]) // 2
    margin = jnp.where((donor == sequence[0]) | (receiver == sequence[0]) | (sizes[receiver] == 0), 0, jnp.maximum(margin, 0))
    moved = jax.random.randint(jax.random.fold_in(own, 4), (number_of // 2,), 0, 1 << 20) % (margin + 1)
    sizes = sizes.at[donor].add(-moved).at[receiver].add(moved)
    members = jnp.searchsorted(jnp.cumsum(sizes), jnp.arange(rows * top), side="right").astype(jnp.int32)
    listing = members.reshape(top, rows).T
    listing = listing[jax.random.permutation(jax.random.fold_in(own, 1), rows)]
    offset_by = jax.random.randint(jax.random.fold_in(own, 2), (rows, 1), 0, top)
    return jnp.take_along_axis(listing, (jnp.arange(top)[None, :] + offset_by) % top, axis=1)


def load_shares(count, total, reach, skew, full):
    portions = [(1 << 20) // math.isqrt(standing ** skew) + 1 for standing in range(1, count + 1)]
    largest = reach if full else min(reach, max(-(-total // count), total * portions[0] // sum(portions)))
    least = 1 if total - largest >= count - 1 else 0
    holding, rest = [largest] + [least] * (count - 1), total - largest - least * (count - 1)
    while rest > 0:
        candidates = [i for i in range(1, count) if holding[i] < largest] or [i for i in range(1, count) if holding[i] < reach]
        whole, budget = sum([portions[i] for i in candidates]), rest
        for i in candidates:
            more = min(reach - holding[i], max(1, budget * portions[i] // whole), rest)
            holding[i] = holding[i] + more
            rest = rest - more
    return np.array(holding)


def centred(key, extent, deviation, reach, cuts=(), kind=jnp.bfloat16):
    drawn = jax.random.normal(key, extent, jnp.float32) * deviation
    if len(cuts) > 0:
        drawn = block_scale(key, extent, cuts, -0.22, 0.18) * drawn
    return jnp.clip(drawn, min=-reach, max=reach).astype(kind)


def setup_inputs(seed: int = 0) -> dict:
    key_list = jax.random.split(jax.random.key(seed), 7)
    tile_slabs = centred(key_list[0], (SUBS, BZ, BY * BX), 1.0, 6.0, ((0, 32),), jnp.float32)
    dest_rank_keys = jax.random.split(jax.random.fold_in(key_list[1], 1), SUBS // SB_DEV)
    dest_rank_turns = jax.random.permutation(jax.random.fold_in(key_list[1], 3), SUBS // SB_DEV)
    dest_rank = jax.vmap(lambda own, number: assign_block(jax.random.fold_in(key_list[1], 2), own, number, SB_DEV, N_ACQ, 1, CAP, 2))(dest_rank_keys, dest_rank_turns).reshape((SUBS, 1))
    block_slot = with_ends(jax.random.randint(key_list[2], (SUBS,), 0, BLOCKS_DEV), jax.random.fold_in(key_list[2], 1), 0, BLOCKS_DEV - 1).astype(jnp.int32)
    shifts = jnp.clip(jax.random.uniform(key_list[3], (SUBS, 3), jnp.float32, 0.0, 1.0), 0.0, 1.0)
    blend_weight = jnp.clip(jnp.exp(jax.random.uniform(key_list[4], (SUBS,), jnp.float32, math.log(0.25), math.log(4.0))), 0.25, 4.0)
    parent_map = with_ends(jax.random.randint(key_list[5], (BLOCKS,), 0, N_GRP * PAR_DEV * 8), jax.random.fold_in(key_list[5], 1), 0, (N_GRP * PAR_DEV * 8) - 1).astype(jnp.int32)
    return {"tile_slabs": tile_slabs, "dest_rank": dest_rank, "block_slot": block_slot, "shifts": shifts, "blend_weight": blend_weight, "parent_map": parent_map}


def resample(blocks, offsets):
    frac_z = offsets[:, 0].reshape(-1, 1, 1, 1)
    frac_y = offsets[:, 1].reshape(-1, 1, 1, 1)
    frac_x = offsets[:, 2].reshape(-1, 1, 1, 1)
    ahead = jnp.concatenate([blocks[:, :, :, 1:], blocks[:, :, :, -1:]], axis=3)
    blocks = (1.0 - frac_x) * blocks + frac_x * ahead
    ahead = jnp.concatenate([blocks[:, :, 1:, :], blocks[:, :, -1:, :]], axis=2)
    blocks = (1.0 - frac_y) * blocks + frac_y * ahead
    ahead = jnp.concatenate([blocks[:, 1:, :, :], blocks[:, -1:, :, :]], axis=1)
    blocks = (1.0 - frac_z) * blocks + frac_z * ahead
    return blocks


def coarsen(blocks):
    count = blocks.shape[0]
    paired = blocks[..., 0::2] + blocks[..., 1::2]
    shaped = paired.reshape(count, BZ // 2, 2, BY // 2, 2, BX // 2)
    summed = jnp.sum(shaped, axis=(2, 4))
    return (0.125 * summed).reshape(count, -1)


def reference(tile_slabs, dest_rank, block_slot, shifts, blend_weight, parent_map):
    volume = jnp.moveaxis(tile_slabs.reshape(N_ACQ, N_GRP, SB_DEV, BZ, BY, BX), 1, 0)
    targets = jnp.moveaxis(dest_rank[:, 0].reshape(N_ACQ, N_GRP, SB_DEV), 1, 0)
    slots = jnp.moveaxis(block_slot.reshape(N_ACQ, N_GRP, SB_DEV), 1, 0)
    offsets = jnp.moveaxis(shifts.reshape(N_ACQ, N_GRP, SB_DEV, 3), 1, 0)
    weights = jnp.moveaxis(blend_weight.reshape(N_ACQ, N_GRP, SB_DEV), 1, 0)

    def one_group(args):
        cells, target, slot, offset, weight = args
        resampled = resample(cells.reshape(N_ACQ * SB_DEV, BZ, BY, BX), offset.reshape(-1, 3))
        place = (target * BLOCKS_DEV + slot).reshape(-1).astype(jnp.int32)
        rows = jnp.arange(N_ACQ * BLOCKS_DEV, dtype=jnp.int32)
        mixing = (rows[:, None] == place[None, :]).astype(jnp.float32) * weight.reshape(1, -1)
        numer = jnp.dot(mixing, resampled.reshape(N_ACQ * SB_DEV, -1), precision=lax.Precision.HIGHEST)
        denom = jnp.sum(mixing, axis=1)
        joined = numer / jnp.maximum(denom, 1.0)[:, None]
        coarse = coarsen(joined.reshape(-1, BZ, BY, BX))
        return coarse.reshape(N_ACQ, BLOCKS_DEV, -1)

    coarse_all = lax.map(one_group, (volume, targets, slots, offsets, weights))
    coarse_all = jnp.moveaxis(coarse_all, 0, 1).reshape(N_ACQ, N_GRP * BLOCKS_DEV, -1)
    parents = parent_map.reshape(N_ACQ, N_GRP * BLOCKS_DEV)

    def one_column(coarse, parent):
        rows = jnp.arange(N_GRP * PAR_DEV * 8, dtype=jnp.int32)
        placing = (rows[:, None] == parent[None, :]).astype(jnp.float32)
        return jnp.dot(placing, coarse, precision=lax.Precision.HIGHEST)

    pyramid = jax.vmap(one_column)(coarse_all, parents)
    return pyramid.reshape(PARENTS, 8, BZ // 2, (BY // 2) * (BX // 2))
```

```python
import functools
import jax
import jax.numpy as jnp
from jax import lax
from jax.experimental import pallas as pl
from jax.experimental.pallas import tpu as pltpu
from jax.sharding import PartitionSpec as P

BZ = 16
BY = 32
BX = 128
PAR_DEV = 2
HZ, HY, HX = BZ // 2, BY // 2, BX // 2
PAIRS = HY // 2
LANES = HY * HX
MESH = pl.DeviceIdType.MESH


def flip(index, mask, count):
    if count & (count - 1):
        return (2 * count + mask - index) % count
    out, bit = index, 1
    while bit < count:
        if mask & bit:
            out = out + bit * (1 - 2 * ((index // bit) % 2))
        bit *= 2
    return out


def partners(count):
    return list(range(1, count)) if count & (count - 1) == 0 else list(range(count))


def halving_matrix():
    row = lax.broadcasted_iota(jnp.int32, (2 * BX, 2 * BX), 0)
    col = lax.broadcasted_iota(jnp.int32, (2 * BX, 2 * BX), 1)
    x, y = row % BX, row // BX
    cx, cy, part = col % HX, (col // HX) % 2, col // BX
    same = y == cy
    both = jnp.where(same & (x // 2 == cx), 1.0, 0.0)
    ahead = jnp.where(same & (x == jnp.minimum(2 * cx + 2, BX - 1)), 1.0, 0.0)
    here = jnp.where(same & (x == 2 * cx), 1.0, 0.0)
    return jnp.where(part == 0, both, ahead - here).astype(jnp.bfloat16)


def split(values):
    high = values.astype(jnp.bfloat16)
    return high, (values - high.astype(jnp.float32)).astype(jnp.bfloat16)


def kernel(
    n_acq, n_grp, cap, scal, source, tile_hbm, slot_lane, parents, out,
    tile, thin, high, low, half, send, gath, pmap,
    load_sem, send_a, recv_a, send_x, recv_x, send_c, recv_c, send_p, recv_p,
):
    count = tile.shape[0]
    a, g = lax.axis_index("acq"), lax.axis_index("grp")
    hi, lo = g // 2, g % 2
    mate = hi * 2 + (1 - lo)
    n_hi = n_grp // 2
    rows = PAIRS * HZ

    barrier = pltpu.get_barrier_semaphore()
    for d in range(1, n_acq):
        pl.semaphore_signal(barrier, inc=1, device_id=((a + d) % n_acq, g), device_id_type=MESH)
    for d in range(1, n_grp):
        pl.semaphore_signal(barrier, inc=1, device_id=(a, (g + d) % n_grp), device_id_type=MESH)

    loads = [pltpu.make_async_copy(tile_hbm.at[s], tile.at[s], load_sem.at[s]) for s in range(count)]
    for load in loads:
        load.start()

    matrix = halving_matrix()
    last = lax.broadcasted_iota(jnp.int32, (HZ, BX), 0) == HZ - 1

    def soften(s, carry):
        pltpu.make_async_copy(tile_hbm.at[s], tile.at[s], load_sem.at[s]).wait()
        fz, fy = scal[s, 0], scal[s, 1]

        def row(y):
            return tile[s, :, pl.ds(y * BX, BX)]

        here = row(0)
        for j in range(HY):
            odd = row(2 * j + 1)
            ahead = row(2 * j + 2) if j < HY - 1 else odd
            thin[s, j] = here + odd + fy * (ahead - here)
            here = ahead
        for j in range(HY):
            even = thin[s, j, pl.ds(0, HZ, stride=2), :]
            odd = thin[s, j, pl.ds(1, HZ, stride=2), :]
            ahead = jnp.where(last, odd, pltpu.roll(even, HZ - 1, 0))
            top, rest = split(even + odd + fz * (ahead - even))
            place = (pl.ds((j // 2) * HZ, HZ), pl.ds((j % 2) * BX, BX))
            high[s, place[0], place[1]] = top.astype(jnp.float32)
            low[s, place[0], place[1]] = rest.astype(jnp.float32)
        return carry

    lax.fori_loop(0, count, soften, 0)

    def halve(s, carry):
        half[s] = jnp.dot(
            high[s].astype(jnp.bfloat16), matrix, preferred_element_type=jnp.float32
        ) + jnp.dot(low[s].astype(jnp.bfloat16), matrix, preferred_element_type=jnp.float32)
        return carry

    lax.fori_loop(0, count, halve, 0, unroll=True)
    half[count] = jnp.zeros((rows, 2 * BX), jnp.float32)

    for place in range(n_acq * cap):
        s = source[place]
        fx, weight = scal[s, 2], scal[s, 3]
        value = weight * (half[s, :, pl.ds(0, BX)] + fx * half[s, :, pl.ds(BX, BX)])
        for p in range(PAIRS):
            send[place // cap, pl.ds((place % cap) * HZ, HZ), pl.ds(p * BX, BX)] = value[
                p * HZ : (p + 1) * HZ
            ]

    pl.semaphore_wait(barrier, n_acq - 1 + n_grp - 1)

    def to_acq(peer):
        return pltpu.make_async_remote_copy(
            src_ref=send.at[peer], dst_ref=gath.at[g, a],
            send_sem=send_a.at[peer], recv_sem=recv_a.at[a],
            device_id=(peer, g), device_id_type=MESH,
        )

    def from_acq(peer):
        return pltpu.make_async_remote_copy(
            src_ref=send.at[peer], dst_ref=gath.at[g, peer],
            send_sem=send_a.at[peer], recv_sem=recv_a.at[peer],
            device_id=(peer, g), device_id_type=MESH,
        )

    def across(owner, k, peer, sends, recvs, at):
        return pltpu.make_async_remote_copy(
            src_ref=gath.at[owner, k], dst_ref=gath.at[owner, k],
            send_sem=sends.at[at, k], recv_sem=recvs.at[owner, k],
            device_id=(a, peer), device_id_type=MESH,
        )

    gath[g, a] = send[a]
    pmap[g] = parents[...]
    order = [flip(a, d, n_acq) for d in range(1, n_acq)]
    for peer in order:
        to_acq(peer).start()
    for d in range(1, n_grp):
        peer = (g + d) % n_grp
        pltpu.make_async_remote_copy(
            src_ref=parents, dst_ref=pmap.at[g], send_sem=send_p.at[d], recv_sem=recv_p.at[g],
            device_id=(a, peer), device_id_type=MESH,
        ).start()

    others = [((hi + d) % n_hi) * 2 + lo for d in range(1, n_hi)]
    origins = [((hi + n_hi - d) % n_hi) * 2 + lo for d in range(1, n_hi)]
    mates = [mate] + [((hi + n_hi - d) % n_hi) * 2 + 1 - lo for d in range(1, n_hi)]

    def forward(k):
        for d, peer in enumerate(others):
            across(g, k, peer, send_x, recv_x, d).start()
        across(g, k, mate, send_c, recv_c, 0).start()

    def relay(k):
        for d, owner in enumerate(origins):
            across(owner, k, mate, send_x, recv_x, d).wait_recv()
            across(owner, k, mate, send_c, recv_c, d + 1).start()

    steps = [a] + order
    for i, k in enumerate(steps):
        if i > 0:
            from_acq(k).wait_recv()
        forward(k)
        if i > 0:
            relay(steps[i - 1])
    relay(steps[-1])

    for d in range(1, n_grp):
        peer = (g + n_grp - d) % n_grp
        pltpu.make_async_remote_copy(
            src_ref=parents, dst_ref=pmap.at[peer], send_sem=send_p.at[d], recv_sem=recv_p.at[peer],
            device_id=(a, peer), device_id_type=MESH,
        ).wait_recv()
    for owner in mates:
        for k in steps:
            across(owner, k, mate, send_c, recv_c, 0).wait_recv()

    depth = n_acq * cap * HZ
    tall = PAR_DEV * 8 * HZ
    lane = lax.broadcasted_iota(jnp.int32, (1, depth), 1)
    spot = lax.broadcasted_iota(jnp.int32, (tall, depth), 0) + g * tall
    blocks = pmap.shape[1]
    places = lax.broadcasted_iota(jnp.int32, (blocks, depth), 0)
    total = None
    for owner in range(n_grp):
        named = jnp.sum(
            jnp.where(slot_lane[pl.ds(owner, 1), :] == places, pmap[owner], 0), axis=0, keepdims=True
        )
        placing = jnp.where(named * HZ + lane % HZ == spot, 1.0, 0.0).astype(jnp.bfloat16)
        top, rest = split(gath[owner].reshape(depth, LANES))
        part = jnp.dot(placing, top, preferred_element_type=jnp.float32) + jnp.dot(
            placing, rest, preferred_element_type=jnp.float32
        )
        total = part if total is None else total + part
    out[...] = total

    for peer in order:
        to_acq(peer).wait_send()
    for d in range(1, n_grp):
        pltpu.make_async_remote_copy(
            src_ref=parents, dst_ref=pmap.at[g], send_sem=send_p.at[d], recv_sem=recv_p.at[g],
            device_id=(a, (g + d) % n_grp), device_id_type=MESH,
        ).wait_send()
    for k in steps:
        for d, peer in enumerate(others):
            across(g, k, peer, send_x, recv_x, d).wait_send()
        across(g, k, mate, send_c, recv_c, 0).wait_send()
        for d, owner in enumerate(origins):
            across(owner, k, mate, send_c, recv_c, d + 1).wait_send()


def body(tile_slabs, dest_rank, block_slot, shifts, blend_weight, parent_map):
    n_acq, n_grp = lax.axis_size("acq"), lax.axis_size("grp")
    a, g = lax.axis_index("acq"), lax.axis_index("grp")
    count = tile_slabs.shape[0]
    blocks = parent_map.shape[0]
    cap = max(2, 2 * count // n_acq)
    shape = (n_acq, n_grp, count)

    def mine(values):
        return lax.dynamic_index_in_dim(values.reshape(shape), g, 1, False)

    dest, slots = dest_rank[:, 0].reshape(shape), block_slot.reshape(shape)
    targets, places, weights = mine(dest), mine(slots), mine(blend_weight)
    own = a * n_grp + g
    offsets = lax.dynamic_index_in_dim(shifts.reshape(n_acq * n_grp, count, 3), own, 0, False)
    own_target = lax.dynamic_index_in_dim(targets, a, 0, False)
    own_place = lax.dynamic_index_in_dim(places, a, 0, False)
    own_weight = lax.dynamic_index_in_dim(weights, a, 0, False)
    key = (targets * blocks + places).reshape(1, -1)
    own_key = (own_target * blocks + own_place).reshape(-1, 1)
    denom = jnp.sum(jnp.where(key == own_key, weights.reshape(1, -1), 0.0), axis=1)
    factor = 0.125 * own_weight / jnp.maximum(denom, 1.0)
    scal = jnp.concatenate([offsets, factor[:, None]], axis=1)
    scal = jnp.concatenate([scal, jnp.zeros((1, 4), jnp.float32)], axis=0)

    index = jnp.arange(count, dtype=jnp.int32)
    earlier = index[None, :] < index[:, None]
    own_order = jnp.sum(
        ((own_target[None, :] == own_target[:, None]) & earlier).astype(jnp.int32), axis=1
    )
    spot = own_target * cap + own_order
    send_rows = jnp.arange(n_acq * cap, dtype=jnp.int32)
    source = count - jnp.sum(
        jnp.where(send_rows[:, None] == spot[None, :], count - index[None, :], 0), axis=1
    )

    here = dest == a
    order = jnp.sum((here[:, :, None, :] & earlier).astype(jnp.int32), axis=3)
    capacity = jnp.arange(cap, dtype=jnp.int32)
    arriving = here[:, :, None, :] & (order[:, :, None, :] == capacity[:, None])
    slot_of = jnp.sum(jnp.where(arriving, slots[:, :, None, :] + 1, 0), axis=3) - 1
    depth = n_acq * cap * HZ
    slot_lane = jnp.repeat(slot_of.transpose(1, 0, 2).reshape(n_grp, n_acq * cap), HZ, axis=1)
    parents = jnp.broadcast_to(parent_map[:, None], (blocks, depth))

    vmem, smem = pl.BlockSpec(memory_space=pltpu.VMEM), pl.BlockSpec(memory_space=pltpu.SMEM)
    rows = PAIRS * HZ
    dma = pltpu.SemaphoreType.DMA
    n_hi = n_grp // 2
    summed = pl.pallas_call(
        functools.partial(kernel, n_acq, n_grp, cap),
        out_shape=jax.ShapeDtypeStruct((PAR_DEV * 8 * HZ, LANES), jnp.float32),
        in_specs=[smem, smem, pl.BlockSpec(memory_space=pl.ANY), vmem, vmem],
        out_specs=vmem,
        scratch_shapes=[
            pltpu.VMEM((count, BZ, BY * BX), jnp.float32),
            pltpu.VMEM((count, HY, BZ, BX), jnp.float32),
            pltpu.VMEM((count, rows, 2 * BX), jnp.float32),
            pltpu.VMEM((count, rows, 2 * BX), jnp.float32),
            pltpu.VMEM((count + 1, rows, 2 * BX), jnp.float32),
            pltpu.VMEM((n_acq, cap * HZ, LANES), jnp.float32),
            pltpu.VMEM((n_grp, n_acq, cap * HZ, LANES), jnp.float32),
            pltpu.VMEM((n_grp, blocks, depth), jnp.int32),
            dma((count,)),
            dma((n_acq,)), dma((n_acq,)),
            dma((max(1, n_hi - 1), n_acq)), dma((n_grp, n_acq)),
            dma((n_hi, n_acq)), dma((n_grp, n_acq)),
            dma((n_grp,)), dma((n_grp,)),
        ],
        compiler_params=pltpu.CompilerParams(collective_id=0, has_side_effects=True),
    )(scal, source, tile_slabs, slot_lane, parents)
    return summed.reshape(PAR_DEV, 8, HZ, LANES)


def solution(mesh):
    placed = (P(("acq", "grp"), None, None), P(), P(), P(), P(), P(("acq", "grp")))
    return jax.shard_map(
        body,
        mesh=mesh,
        in_specs=placed,
        out_specs=P(("acq", "grp"), None, None, None),
        check_vma=False,
    )
```

```python
import functools
import jax
import jax.numpy as jnp
from jax import lax
from jax.experimental import pallas as pl
from jax.experimental.pallas import tpu as pltpu
from jax.sharding import PartitionSpec as P

BZ = 16
BY = 32
BX = 128
PAR_DEV = 2
HZ, HY, HX = BZ // 2, BY // 2, BX // 2
PAIRS = HY // 2
LANES = HY * HX
VMEM_LIMIT = 62
MESH = pl.DeviceIdType.MESH


def flip(index, mask, count):
    if count & (count - 1):
        return (2 * count + mask - index) % count
    out, bit = index, 1
    while bit < count:
        if mask & bit:
            out = out + bit * (1 - 2 * ((index // bit) % 2))
        bit *= 2
    return out


def partners(count):
    return list(range(1, count)) if count & (count - 1) == 0 else list(range(count))


def halving_matrix():
    row = lax.broadcasted_iota(jnp.int32, (2 * BX, 2 * BX), 0)
    col = lax.broadcasted_iota(jnp.int32, (2 * BX, 2 * BX), 1)
    x, y = row % BX, row // BX
    cx, cy, part = col % HX, (col // HX) % 2, col // BX
    same = y == cy
    both = jnp.where(same & (x // 2 == cx), 1.0, 0.0)
    ahead = jnp.where(same & (x == jnp.minimum(2 * cx + 2, BX - 1)), 1.0, 0.0)
    here = jnp.where(same & (x == 2 * cx), 1.0, 0.0)
    return jnp.where(part == 0, both, ahead - here).astype(jnp.bfloat16)


def split(values):
    high = values.astype(jnp.bfloat16)
    return high, (values - high.astype(jnp.float32)).astype(jnp.bfloat16)


def kernel(
    n_acq, n_grp, cap, tile_hbm, dest_hbm, slot_hbm, weight_hbm, shift_hbm, parent_hbm, out,
    dest, slot, weight, shift, parent, dest_row, slot_row, weight_row,
    tile, thin, high, low, half, factor, send, gath, named,
    meta_sem, load_sem, send_a, recv_a, send_x, recv_x, send_c, recv_c, send_p, recv_p,
):
    count = tile.shape[0]
    a, g = lax.axis_index("acq"), lax.axis_index("grp")
    hi, lo = g // 2, g % 2
    mate = hi * 2 + (1 - lo)
    n_hi = n_grp // 2
    rows = PAIRS * HZ

    barrier = pltpu.get_barrier_semaphore()
    for d in range(1, n_acq):
        pl.semaphore_signal(barrier, inc=1, device_id=((a + d) % n_acq, g), device_id_type=MESH)
    for d in range(1, n_grp):
        pl.semaphore_signal(barrier, inc=1, device_id=(a, (g + d) % n_grp), device_id_type=MESH)

    metas = [
        pltpu.make_async_copy(start, end, meta_sem.at[i])
        for i, (start, end) in enumerate((
            (dest_hbm, dest), (slot_hbm, slot), (weight_hbm, weight), (shift_hbm, shift),
            (parent_hbm, parent), (dest_hbm, dest_row), (slot_hbm, slot_row), (weight_hbm, weight_row),
        ))
    ]
    for meta in metas:
        meta.start()
    loads = [pltpu.make_async_copy(tile_hbm.at[s], tile.at[s], load_sem.at[s]) for s in range(count)]
    for load in loads:
        load.start()

    matrix = halving_matrix()
    last = lax.broadcasted_iota(jnp.int32, (HZ, BX), 0) == HZ - 1
    for meta in metas:
        meta.wait()

    blocks = parent.shape[1]
    base = (a * n_grp + g) * count
    target = [dest[0, base + s] for s in range(count)]
    key = [target[s] * blocks + slot[0, base + s] for s in range(count)]
    subs = lax.broadcasted_iota(jnp.int32, dest_row.shape, 1)
    keys = jnp.where(
        (subs // count) % n_grp == g, dest_row[...] * blocks + slot_row[...], -1
    )
    for s in range(count):
        denom = jnp.sum(jnp.where(keys == key[s], weight_row[...], 0.0), axis=1, keepdims=True)
        factor[s] = jnp.broadcast_to(
            (0.125 * weight[0, base + s]) / jnp.maximum(denom, 1.0), (HZ, BX)
        )
    factor[count] = jnp.zeros((HZ, BX), jnp.float32)
    spot = []
    for s in range(count):
        at = target[s] * cap
        for before in range(s):
            at = at + jnp.where(target[before] == target[s], 1, 0)
        spot.append(at)

    def soften(s, carry):
        pltpu.make_async_copy(tile_hbm.at[s], tile.at[s], load_sem.at[s]).wait()
        fz, fy = shift[0, base + s], shift[1, base + s]

        def row(y):
            return tile[s, :, pl.ds(y * BX, BX)]

        here = row(0)
        for j in range(HY):
            odd = row(2 * j + 1)
            ahead = row(2 * j + 2) if j < HY - 1 else odd
            thin[s, j] = here + odd + fy * (ahead - here)
            here = ahead
        for j in range(HY):
            even = thin[s, j, pl.ds(0, HZ, stride=2), :]
            odd = thin[s, j, pl.ds(1, HZ, stride=2), :]
            ahead = jnp.where(last, odd, pltpu.roll(even, HZ - 1, 0))
            top, rest = split(even + odd + fz * (ahead - even))
            place = (pl.ds((j // 2) * HZ, HZ), pl.ds((j % 2) * BX, BX))
            high[s, place[0], place[1]] = top.astype(jnp.float32)
            low[s, place[0], place[1]] = rest.astype(jnp.float32)
        return carry

    lax.fori_loop(0, count, soften, 0)

    def halve(s, carry):
        half[s] = jnp.dot(
            high[s].astype(jnp.bfloat16), matrix, preferred_element_type=jnp.float32
        ) + jnp.dot(low[s].astype(jnp.bfloat16), matrix, preferred_element_type=jnp.float32)
        return carry

    lax.fori_loop(0, count, halve, 0, unroll=True)
    half[count] = jnp.zeros((rows, 2 * BX), jnp.float32)

    for place in range(n_acq * cap):
        s = count
        for i in range(count):
            s = jnp.where(spot[i] == place, i, s)
        fx = shift[2, base + jnp.minimum(s, count - 1)]
        value = half[s, :, pl.ds(0, BX)] + fx * half[s, :, pl.ds(BX, BX)]
        scale = factor[s]
        for p in range(PAIRS):
            send[place // cap, pl.ds((place % cap) * HZ, HZ), pl.ds(p * BX, BX)] = scale * value[
                p * HZ : (p + 1) * HZ
            ]

    pl.semaphore_wait(barrier, n_acq - 1 + n_grp - 1)

    def to_acq(peer):
        return pltpu.make_async_remote_copy(
            src_ref=send.at[peer], dst_ref=gath.at[g, a],
            send_sem=send_a.at[peer], recv_sem=recv_a.at[a],
            device_id=(peer, g), device_id_type=MESH,
        )

    def from_acq(peer):
        return pltpu.make_async_remote_copy(
            src_ref=send.at[peer], dst_ref=gath.at[g, peer],
            send_sem=send_a.at[peer], recv_sem=recv_a.at[peer],
            device_id=(peer, g), device_id_type=MESH,
        )

    def across(owner, k, peer, sends, recvs, at):
        return pltpu.make_async_remote_copy(
            src_ref=gath.at[owner, k], dst_ref=gath.at[owner, k],
            send_sem=sends.at[at, k], recv_sem=recvs.at[owner, k],
            device_id=(a, peer), device_id_type=MESH,
        )

    gath[g, a] = send[a]
    order = [flip(a, d, n_acq) for d in partners(n_acq)]
    for peer in order:
        to_acq(peer).start()

    others = [((hi + d) % n_hi) * 2 + lo for d in range(1, n_hi)]
    origins = [((hi + n_hi - d) % n_hi) * 2 + lo for d in range(1, n_hi)]
    mates = [mate] + [((hi + n_hi - d) % n_hi) * 2 + 1 - lo for d in range(1, n_hi)]

    def forward(k):
        for d, peer in enumerate(others):
            across(g, k, peer, send_x, recv_x, d).start()
        across(g, k, mate, send_c, recv_c, 0).start()

    def relay(k):
        for d, owner in enumerate(origins):
            across(owner, k, mate, send_x, recv_x, d).wait_recv()
            across(owner, k, mate, send_c, recv_c, d + 1).start()

    depth = n_acq * cap * HZ
    tall = PAR_DEV * 8 * HZ
    lane = lax.broadcasted_iota(jnp.int32, (HZ, depth), 1)

    def name(k, found):
        first = (k * n_grp + g) * count
        seen = 0
        slots = [0] * cap
        for s in range(count):
            hit = jnp.where(dest[0, first + s] == a, 1, 0)
            for c in range(cap):
                slots[c] = jnp.where(
                    (hit == 1) & (seen == c), slot[0, first + s], slots[c]
                )
            seen = seen + hit
        for c in range(cap):
            found = jnp.where(lane // HZ == k * cap + c, parent[0, slots[c]], found)
        return found

    steps = [a] + order
    forward(a)
    named[g] = lax.fori_loop(0, n_acq, name, jnp.zeros((HZ, depth), jnp.int32))

    def telling(d, owner, peer):
        return pltpu.make_async_remote_copy(
            src_ref=named.at[owner], dst_ref=named.at[owner],
            send_sem=send_p.at[d], recv_sem=recv_p.at[owner],
            device_id=(a, peer), device_id_type=MESH,
        )

    for d in range(1, n_grp):
        telling(d, g, (g + d) % n_grp).start()

    upright = lax.broadcasted_iota(jnp.int32, (tall, depth), 0) + g * tall
    across_lane = lax.broadcasted_iota(jnp.int32, (tall, depth), 1) % HZ

    def place_rows(owner):
        placing = jnp.where(
            named[owner, pl.ds(0, 1), :] * HZ + across_lane == upright, 1.0, 0.0
        ).astype(jnp.bfloat16)
        top, rest = split(gath[owner].reshape(depth, LANES))
        return jnp.dot(placing, top, preferred_element_type=jnp.float32) + jnp.dot(
            placing, rest, preferred_element_type=jnp.float32
        )

    for i in range(1, n_acq):
        from_acq(steps[i]).wait_recv()
        forward(steps[i])
        relay(steps[i - 1])
    out[...] = place_rows(g)
    for d in range(1, n_grp):
        owner = (g + n_grp - d) % n_grp
        telling(d, owner, owner).wait_recv()
    for k in steps:
        across(mate, k, mate, send_c, recv_c, 0).wait_recv()
    out[...] += place_rows(mate)
    relay(steps[-1])
    for owner in origins:
        out[...] += place_rows(owner)
    for owner in mates[1:]:
        for k in steps:
            across(owner, k, mate, send_c, recv_c, 0).wait_recv()
        out[...] += place_rows(owner)

    for peer in order:
        to_acq(peer).wait_send()
    for d in range(1, n_grp):
        telling(d, g, (g + d) % n_grp).wait_send()
    for k in steps:
        for d, peer in enumerate(others):
            across(g, k, peer, send_x, recv_x, d).wait_send()
        across(g, k, mate, send_c, recv_c, 0).wait_send()
        for d, owner in enumerate(origins):
            across(owner, k, mate, send_c, recv_c, d + 1).wait_send()


def body(tile_slabs, dest_rank, block_slot, shifts, blend_weight, parent_map):
    n_acq, n_grp = lax.axis_size("acq"), lax.axis_size("grp")
    count = tile_slabs.shape[0]
    subs = dest_rank.shape[0]
    blocks = parent_map.shape[0]
    cap = max(2, 2 * count // n_acq)
    depth = n_acq * cap * HZ
    hbm = pl.BlockSpec(memory_space=pltpu.HBM)
    rows = PAIRS * HZ
    dma = pltpu.SemaphoreType.DMA
    n_hi = n_grp // 2
    summed = pl.pallas_call(
        functools.partial(kernel, n_acq, n_grp, cap),
        out_shape=jax.ShapeDtypeStruct((PAR_DEV * 8 * HZ, LANES), jnp.float32),
        in_specs=[hbm] * 6,
        out_specs=pl.BlockSpec(memory_space=pltpu.VMEM),
        scratch_shapes=[
            pltpu.SMEM((1, subs), jnp.int32),
            pltpu.SMEM((1, subs), jnp.int32),
            pltpu.SMEM((1, subs), jnp.float32),
            pltpu.SMEM((3, subs), jnp.float32),
            pltpu.SMEM((1, blocks), jnp.int32),
            pltpu.VMEM((1, subs), jnp.int32),
            pltpu.VMEM((1, subs), jnp.int32),
            pltpu.VMEM((1, subs), jnp.float32),
            pltpu.VMEM((count, BZ, BY * BX), jnp.float32),
            pltpu.VMEM((count, HY, BZ, BX), jnp.float32),
            pltpu.VMEM((count, rows, 2 * BX), jnp.float32),
            pltpu.VMEM((count, rows, 2 * BX), jnp.float32),
            pltpu.VMEM((count + 1, rows, 2 * BX), jnp.float32),
            pltpu.VMEM((count + 1, HZ, BX), jnp.float32),
            pltpu.VMEM((n_acq, cap * HZ, LANES), jnp.float32),
            pltpu.VMEM((n_grp, n_acq, cap * HZ, LANES), jnp.float32),
            pltpu.VMEM((n_grp, HZ, depth), jnp.int32),
            dma((8,)), dma((count,)),
            dma((n_acq,)), dma((n_acq,)),
            dma((max(1, n_hi - 1), n_acq)), dma((n_grp, n_acq)),
            dma((n_hi, n_acq)), dma((n_grp, n_acq)),
            dma((n_grp,)), dma((n_grp,)),
        ],
        compiler_params=pltpu.CompilerParams(
            collective_id=0, has_side_effects=True, vmem_limit_bytes=VMEM_LIMIT * 2**20
        ),
    )(
        tile_slabs, dest_rank.reshape(1, subs), block_slot.reshape(1, subs),
        blend_weight.reshape(1, subs), shifts.T, parent_map.reshape(1, blocks),
    )
    return summed.reshape(PAR_DEV, 8, HZ, LANES)


def solution(mesh):
    placed = (P(("acq", "grp"), None, None), P(), P(), P(), P(), P(("acq", "grp")))
    return jax.shard_map(
        body,
        mesh=mesh,
        in_specs=placed,
        out_specs=P(("acq", "grp"), None, None, None),
        check_vma=False,
    )
```

```python
import functools
import jax
import jax.numpy as jnp
from jax import lax
from jax.experimental import pallas as pl
from jax.experimental.pallas import tpu as pltpu
from jax.sharding import PartitionSpec as P

BZ = 16
BY = 32
BX = 128
PAR_DEV = 2
HZ, HY, HX = BZ // 2, BY // 2, BX // 2
PAIRS = HY // 2
LANES = HY * HX
VMEM_LIMIT = 62
MESH = pl.DeviceIdType.MESH


def flip(index, mask, count):
    if count & (count - 1):
        return (2 * count + mask - index) % count
    out, bit = index, 1
    while bit < count:
        if mask & bit:
            out = out + bit * (1 - 2 * ((index // bit) % 2))
        bit *= 2
    return out


def partners(count):
    return list(range(1, count)) if count & (count - 1) == 0 else list(range(count))


def halving_matrix():
    row = lax.broadcasted_iota(jnp.int32, (2 * BX, 2 * BX), 0)
    col = lax.broadcasted_iota(jnp.int32, (2 * BX, 2 * BX), 1)
    x, y = row % BX, row // BX
    cx, cy, part = col % HX, (col // HX) % 2, col // BX
    same = y == cy
    both = jnp.where(same & (x // 2 == cx), 1.0, 0.0)
    ahead = jnp.where(same & (x == jnp.minimum(2 * cx + 2, BX - 1)), 1.0, 0.0)
    here = jnp.where(same & (x == 2 * cx), 1.0, 0.0)
    return jnp.where(part == 0, both, ahead - here).astype(jnp.bfloat16)


def split(values):
    high = values.astype(jnp.bfloat16)
    return high, (values - high.astype(jnp.float32)).astype(jnp.bfloat16)


def kernel(
    n_acq, n_grp, cap, tile_hbm, dest_hbm, slot_hbm, weight_hbm, shift_hbm, parent_hbm, out,
    dest, slot, weight, shift, parent, dest_row, slot_row, weight_row,
    tile, thin, high, low, half, factor, send, gath, named,
    meta_sem, load_sem, send_a, recv_a, send_x, recv_x, send_c, recv_c, send_p, recv_p,
):
    count = tile.shape[0]
    a, g = lax.axis_index("acq"), lax.axis_index("grp")
    hi, lo = g // 2, g % 2
    mate = hi * 2 + (1 - lo)
    n_hi = n_grp // 2
    rows = PAIRS * HZ

    barrier = pltpu.get_barrier_semaphore()
    for d in range(1, n_acq):
        pl.semaphore_signal(barrier, inc=1, device_id=((a + d) % n_acq, g), device_id_type=MESH)
    for d in range(1, n_grp):
        pl.semaphore_signal(barrier, inc=1, device_id=(a, (g + d) % n_grp), device_id_type=MESH)

    metas = [
        pltpu.make_async_copy(start, end, meta_sem.at[i])
        for i, (start, end) in enumerate((
            (dest_hbm, dest), (slot_hbm, slot), (weight_hbm, weight), (shift_hbm, shift),
            (parent_hbm, parent), (dest_hbm, dest_row), (slot_hbm, slot_row), (weight_hbm, weight_row),
        ))
    ]
    for meta in metas:
        meta.start()
    loads = [pltpu.make_async_copy(tile_hbm.at[s], tile.at[s], load_sem.at[s]) for s in range(count)]
    for load in loads:
        load.start()

    matrix = halving_matrix()
    last = lax.broadcasted_iota(jnp.int32, (HZ, BX), 0) == HZ - 1
    for meta in metas:
        meta.wait()

    blocks = parent.shape[1]
    base = (a * n_grp + g) * count
    target = [dest[0, base + s] for s in range(count)]
    key = [target[s] * blocks + slot[0, base + s] for s in range(count)]
    subs = lax.broadcasted_iota(jnp.int32, dest_row.shape, 1)
    keys = jnp.where(
        (subs // count) % n_grp == g, dest_row[...] * blocks + slot_row[...], -1
    )
    for s in range(count):
        denom = jnp.sum(jnp.where(keys == key[s], weight_row[...], 0.0), axis=1, keepdims=True)
        factor[s] = jnp.broadcast_to(
            (0.125 * weight[0, base + s]) / jnp.maximum(denom, 1.0), (HZ, BX)
        )
    factor[count] = jnp.zeros((HZ, BX), jnp.float32)
    spot = []
    for s in range(count):
        at = target[s] * cap
        for before in range(s):
            at = at + jnp.where(target[before] == target[s], 1, 0)
        spot.append(at)

    def soften(s, carry):
        pltpu.make_async_copy(tile_hbm.at[s], tile.at[s], load_sem.at[s]).wait()
        fz, fy = shift[0, base + s], shift[1, base + s]

        def row(y):
            return tile[s, :, pl.ds(y * BX, BX)]

        here = row(0)
        for j in range(HY):
            odd = row(2 * j + 1)
            ahead = row(2 * j + 2) if j < HY - 1 else odd
            thin[s, j] = here + odd + fy * (ahead - here)
            here = ahead
        for j in range(HY):
            even = thin[s, j, pl.ds(0, HZ, stride=2), :]
            odd = thin[s, j, pl.ds(1, HZ, stride=2), :]
            ahead = jnp.where(last, odd, pltpu.roll(even, HZ - 1, 0))
            top, rest = split(even + odd + fz * (ahead - even))
            place = (pl.ds((j // 2) * HZ, HZ), pl.ds((j % 2) * BX, BX))
            high[s, place[0], place[1]] = top.astype(jnp.float32)
            low[s, place[0], place[1]] = rest.astype(jnp.float32)
        return carry

    lax.fori_loop(0, count, soften, 0)

    def halve(s, carry):
        half[s] = jnp.dot(
            high[s].astype(jnp.bfloat16), matrix, preferred_element_type=jnp.float32
        ) + jnp.dot(low[s].astype(jnp.bfloat16), matrix, preferred_element_type=jnp.float32)
        return carry

    lax.fori_loop(0, count, halve, 0, unroll=True)
    half[count] = jnp.zeros((rows, 2 * BX), jnp.float32)

    for place in range(n_acq * cap):
        s = count
        for i in range(count):
            s = jnp.where(spot[i] == place, i, s)
        fx = shift[2, base + jnp.minimum(s, count - 1)]
        value = half[s, :, pl.ds(0, BX)] + fx * half[s, :, pl.ds(BX, BX)]
        scale = factor[s]
        for p in range(PAIRS):
            send[place // cap, pl.ds((place % cap) * HZ, HZ), pl.ds(p * BX, BX)] = scale * value[
                p * HZ : (p + 1) * HZ
            ]

    pl.semaphore_wait(barrier, n_acq - 1 + n_grp - 1)

    def to_acq(peer):
        return pltpu.make_async_remote_copy(
            src_ref=send.at[peer], dst_ref=gath.at[g, a],
            send_sem=send_a.at[peer], recv_sem=recv_a.at[a],
            device_id=(peer, g), device_id_type=MESH,
        )

    def from_acq(peer):
        return pltpu.make_async_remote_copy(
            src_ref=send.at[peer], dst_ref=gath.at[g, peer],
            send_sem=send_a.at[peer], recv_sem=recv_a.at[peer],
            device_id=(peer, g), device_id_type=MESH,
        )

    def across(owner, part, peer, sends, recvs, at):
        first, size = parts[part][1:]
        rows_ref = gath.at[owner, pl.ds(first, size)]
        return pltpu.make_async_remote_copy(
            src_ref=rows_ref, dst_ref=rows_ref,
            send_sem=sends.at[at, part], recv_sem=recvs.at[owner, part],
            device_id=(a, peer), device_id_type=MESH,
        )

    gath[g, a] = send[a]
    order = [flip(a, d, n_acq) for d in partners(n_acq)]
    for peer in order:
        to_acq(peer).start()

    steps = [a] + order
    parts = []
    for i, k in enumerate(steps):
        if i < 2 or n_acq & (n_acq - 1):
            parts.append(([i], k, 1))
        elif i % 2 == 1:
            parts.append(([i - 1, i], (k // 2) * 2, 2))

    others = [((hi + d) % n_hi) * 2 + lo for d in range(1, n_hi)]
    origins = [((hi + n_hi - d) % n_hi) * 2 + lo for d in range(1, n_hi)]
    mates = [mate] + [((hi + n_hi - d) % n_hi) * 2 + 1 - lo for d in range(1, n_hi)]

    def forward(k):
        for d, peer in enumerate(others):
            across(g, k, peer, send_x, recv_x, d).start()
        across(g, k, mate, send_c, recv_c, 0).start()

    def relay(k):
        for d, owner in enumerate(origins):
            across(owner, k, mate, send_x, recv_x, d).wait_recv()
            across(owner, k, mate, send_c, recv_c, d + 1).start()

    depth = n_acq * cap * HZ
    tall = PAR_DEV * 8 * HZ
    lane = lax.broadcasted_iota(jnp.int32, (HZ, depth), 1)

    def name(k, found):
        first = (k * n_grp + g) * count
        seen = 0
        slots = [0] * cap
        for s in range(count):
            hit = jnp.where(dest[0, first + s] == a, 1, 0)
            for c in range(cap):
                slots[c] = jnp.where(
                    (hit == 1) & (seen == c), slot[0, first + s], slots[c]
                )
            seen = seen + hit
        for c in range(cap):
            found = jnp.where(lane // HZ == k * cap + c, parent[0, slots[c]], found)
        return found

    forward(0)
    named[g] = lax.fori_loop(0, n_acq, name, jnp.zeros((HZ, depth), jnp.int32))

    def telling(d, owner, peer):
        return pltpu.make_async_remote_copy(
            src_ref=named.at[owner], dst_ref=named.at[owner],
            send_sem=send_p.at[d], recv_sem=recv_p.at[owner],
            device_id=(a, peer), device_id_type=MESH,
        )

    for d in range(1, n_grp):
        telling(d, g, (g + d) % n_grp).start()

    upright = lax.broadcasted_iota(jnp.int32, (tall, depth), 0) + g * tall
    across_lane = lax.broadcasted_iota(jnp.int32, (tall, depth), 1) % HZ

    def place_rows(owner):
        placing = jnp.where(
            named[owner, pl.ds(0, 1), :] * HZ + across_lane == upright, 1.0, 0.0
        ).astype(jnp.bfloat16)
        top, rest = split(gath[owner].reshape(depth, LANES))
        return jnp.dot(placing, top, preferred_element_type=jnp.float32) + jnp.dot(
            placing, rest, preferred_element_type=jnp.float32
        )

    for part in range(1, len(parts)):
        for i in parts[part][0]:
            from_acq(steps[i]).wait_recv()
        forward(part)
        relay(part - 1)
    out[...] = place_rows(g)
    for d in range(1, n_grp):
        owner = (g + n_grp - d) % n_grp
        telling(d, owner, owner).wait_recv()
    for k in range(len(parts)):
        across(mate, k, mate, send_c, recv_c, 0).wait_recv()
    out[...] += place_rows(mate)
    relay(len(parts) - 1)
    for owner in origins:
        out[...] += place_rows(owner)
    for owner in mates[1:]:
        for k in range(len(parts)):
            across(owner, k, mate, send_c, recv_c, 0).wait_recv()
        out[...] += place_rows(owner)

    for peer in order:
        to_acq(peer).wait_send()
    for d in range(1, n_grp):
        telling(d, g, (g + d) % n_grp).wait_send()
    for k in range(len(parts)):
        for d, peer in enumerate(others):
            across(g, k, peer, send_x, recv_x, d).wait_send()
        across(g, k, mate, send_c, recv_c, 0).wait_send()
        for d, owner in enumerate(origins):
            across(owner, k, mate, send_c, recv_c, d + 1).wait_send()


def body(tile_slabs, dest_rank, block_slot, shifts, blend_weight, parent_map):
    n_acq, n_grp = lax.axis_size("acq"), lax.axis_size("grp")
    count = tile_slabs.shape[0]
    subs = dest_rank.shape[0]
    blocks = parent_map.shape[0]
    cap = max(2, 2 * count // n_acq)
    depth = n_acq * cap * HZ
    hbm = pl.BlockSpec(memory_space=pltpu.HBM)
    rows = PAIRS * HZ
    dma = pltpu.SemaphoreType.DMA
    n_hi = n_grp // 2
    summed = pl.pallas_call(
        functools.partial(kernel, n_acq, n_grp, cap),
        out_shape=jax.ShapeDtypeStruct((PAR_DEV * 8 * HZ, LANES), jnp.float32),
        in_specs=[hbm] * 6,
        out_specs=pl.BlockSpec(memory_space=pltpu.VMEM),
        scratch_shapes=[
            pltpu.SMEM((1, subs), jnp.int32),
            pltpu.SMEM((1, subs), jnp.int32),
            pltpu.SMEM((1, subs), jnp.float32),
            pltpu.SMEM((3, subs), jnp.float32),
            pltpu.SMEM((1, blocks), jnp.int32),
            pltpu.VMEM((1, subs), jnp.int32),
            pltpu.VMEM((1, subs), jnp.int32),
            pltpu.VMEM((1, subs), jnp.float32),
            pltpu.VMEM((count, BZ, BY * BX), jnp.float32),
            pltpu.VMEM((count, HY, BZ, BX), jnp.float32),
            pltpu.VMEM((count, rows, 2 * BX), jnp.float32),
            pltpu.VMEM((count, rows, 2 * BX), jnp.float32),
            pltpu.VMEM((count + 1, rows, 2 * BX), jnp.float32),
            pltpu.VMEM((count + 1, HZ, BX), jnp.float32),
            pltpu.VMEM((n_acq, cap * HZ, LANES), jnp.float32),
            pltpu.VMEM((n_grp, n_acq, cap * HZ, LANES), jnp.float32),
            pltpu.VMEM((n_grp, HZ, depth), jnp.int32),
            dma((8,)), dma((count,)),
            dma((n_acq,)), dma((n_acq,)),
            dma((max(1, n_hi - 1), n_acq)), dma((n_grp, n_acq)),
            dma((n_hi, n_acq)), dma((n_grp, n_acq)),
            dma((n_grp,)), dma((n_grp,)),
        ],
        compiler_params=pltpu.CompilerParams(
            collective_id=0, has_side_effects=True, vmem_limit_bytes=VMEM_LIMIT * 2**20
        ),
    )(
        tile_slabs, dest_rank.reshape(1, subs), block_slot.reshape(1, subs),
        blend_weight.reshape(1, subs), shifts.T, parent_map.reshape(1, blocks),
    )
    return summed.reshape(PAR_DEV, 8, HZ, LANES)


def solution(mesh):
    placed = (P(("acq", "grp"), None, None), P(), P(), P(), P(), P(("acq", "grp")))
    return jax.shard_map(
        body,
        mesh=mesh,
        in_specs=placed,
        out_specs=P(("acq", "grp"), None, None, None),
        check_vma=False,
    )
```
